128 devices in a mesh: row: 8 (over x, core), col: 16 (over z, y).
Axes of the slice: x: 4, y: 4, z: 4, core: 2. Of those that a mesh axis runs over, the one named last changes fastest.
Arguments:
- stored: float32 [16384, 16384], P('row', 'col'), as said below
Outputs:
- updated: float32 [16384, 16384], P('row', 'col')
- log_det: float32 [], replicated
Inputs may be any that keep to these rules, and one draw needn't show every extreme that they name: `stored`: read back into global order, the matrix is symmetric positive definite, with every eigenvalue at least 1.
All inputs are finite; a program needn't handle non-finite values.
Results may differ from the reference program's by a relative error of at most 0.0001.
Values sent between devices are 32-bit elements; how exact they have to be, the bound alone decides.
No kernel may reach another device: no remote copies, remote signals or barrier semaphores. Data moves between devices by JAX's collectives and lax.ppermute only.
A program may use at most 256 MiB of HBM per device.

```python
import math
import jax
import jax.numpy as jnp
from jax import lax

N = 16384
NB = 512
PANELS = 2
N_ROW = 8
N_COL = 16


def to_storage(matrix):
    row_blocks = N // NB // N_ROW
    col_blocks = N // NB // N_COL
    shaped = matrix.reshape(row_blocks, N_ROW, NB, col_blocks, N_COL, NB)
    return shaped.transpose(1, 0, 2, 4, 3, 5).reshape(N, N)


def draw_stored(key, part):
    base_key = jax.random.fold_in(key, 7)
    first_key, second_key = jax.random.split(base_key)
    rank_count = N // 8
    factors = jax.random.normal(first_key, (N, rank_count), jnp.float32)
    weights = jnp.exp(jax.random.uniform(second_key, (rank_count,), jnp.float32, math.log(0.25), math.log(1.25)))
    scaled = factors * (weights / rank_count)[None, :]
    coupling = jnp.dot(scaled, factors.T, precision=lax.Precision.HIGHEST, preferred_element_type=jnp.float32)
    coupling = 0.5 * (coupling + coupling.T)
    return to_storage(coupling + jnp.eye(N, dtype=jnp.float32))


def setup_inputs(seed: int = 0) -> dict:
    key_of = jax.random.split(jax.random.key(seed), 2)
    stored = draw_stored(jax.random.fold_in(key_of[1], 71), 0)
    return dict(stored=stored)


def unpermute(stored):
    row_blocks = N // NB // N_ROW
    col_blocks = N // NB // N_COL
    shaped = stored.reshape(N_ROW, row_blocks, NB, N_COL, col_blocks, NB)
    return shaped.transpose(1, 0, 2, 4, 3, 5).reshape(N, N)

def permute(matrix):
    row_blocks = N // NB // N_ROW
    col_blocks = N // NB // N_COL
    shaped = matrix.reshape(row_blocks, N_ROW, NB, col_blocks, N_COL, NB)
    return shaped.transpose(1, 0, 2, 4, 3, 5).reshape(N, N)

def reference(stored):
    matrix = unpermute(stored)
    identity = jnp.eye(NB, dtype=jnp.float32)
    log_total = jnp.zeros((), jnp.float32)
    for number in range(PANELS):
        start = number * NB
        finish = start + NB
        factor = jnp.linalg.cholesky(matrix[start:finish, start:finish])
        inverse = jax.scipy.linalg.solve_triangular(factor, identity, lower=True)
        solved = jnp.dot(matrix[finish:, start:finish].astype(jnp.float32), inverse.T.astype(jnp.float32), precision=lax.Precision.HIGHEST, preferred_element_type=jnp.float32)
        log_total = log_total + 2.0 * jnp.sum(jnp.log(jnp.diagonal(factor)))
        update = jnp.dot(solved.astype(jnp.float32), solved.T.astype(jnp.float32), precision=lax.Precision.HIGHEST, preferred_element_type=jnp.float32)
        matrix = matrix.at[finish:, finish:].add(-update)
        matrix = matrix.at[start:finish, start:finish].set(factor)
        matrix = matrix.at[finish:, start:finish].set(solved)
        matrix = matrix.at[start:finish, finish:].set(0.0)
    return (permute(matrix), log_total)
```

```python
import jax
import jax.numpy as jnp
from jax import lax
from jax.experimental import pallas as pl
from jax.experimental.pallas import tpu as pltpu
from jax.sharding import PartitionSpec as P

NB = 512
TILE = 128
NX, NY, NZ = 4, 4, 4
HI = lax.Precision.HIGHEST
NN = (((1,), (0,)), ((), ()))
TN = (((0,), (0,)), ((), ()))
VMEM_LIMIT = 60 * 2**20


def mm(a, b, dims=NN):
    return lax.dot_general(a, b, dims, precision=HI, preferred_element_type=jnp.float32)


def device(x, core, z, y):
    return (2 * x + core) * (NZ * NY) + z * NY + y


def send(value, pairs):
    return lax.ppermute(value, ("row", "col"), pairs)


def scatter_x(chunks, ys):
    return [
        send(chunks[t], [(device(0, k, z, y), device(t, k, z, y)) for k in range(2) for z, y in ys])
        for t in range(1, NX)
    ]


def spread_y(value, cores, source):
    return [
        send(
            value,
            [(device(x, k, 0, source), device(x, k, 0, (source + t) % NY)) for x in range(NX) for k in cores],
        )
        for t in range(1, NY)
    ]


def spread_z(value, cores):
    return [
        send(
            value,
            [(device(x, k, 0, y), device(x, k, t, y)) for x in range(NX) for k in cores for y in range(NY)],
        )
        for t in range(1, NZ)
    ]


def gather_x(value, cores):
    return [value] + [
        send(
            value,
            [
                (device(x, k, z, y), device((x + t) % NX, k, z, y))
                for x in range(NX)
                for k in cores
                for z in range(NZ)
                for y in range(NY)
            ],
        )
        for t in range(1, NX)
    ]


def swap_core(value, cores):
    return send(
        value,
        [
            (device(x, k, z, y), device(x, 1 - k, z, y))
            for x in range(NX)
            for k in cores
            for z in range(NZ)
            for y in range(NY)
        ],
    )


def pick(mine, own, received):
    total = received[0]
    for other in received[1:]:
        total = total + other
    return jnp.where(mine, own, total)


def spread(x):
    return jnp.broadcast_to(x, (8, TILE))


def factor_tile(a):
    sub = lax.broadcasted_iota(jnp.int32, (8, TILE), 0)
    lane = lax.broadcasted_iota(jnp.int32, (8, TILE), 1)
    groups = TILE // 8
    rows = [a[8 * g : 8 * g + 8, :] for g in range(groups)]
    inv = [jnp.where(lane == sub + 8 * g, 1.0, 0.0).astype(jnp.float32) for g in range(groups)]
    uppers, inverses = [], []
    for b in range(groups):
        v, y = rows[b], inv[b]
        c = [spread(v[:, 8 * b + m : 8 * b + m + 1]) for m in range(8)]
        upper, inverse = jnp.zeros_like(v), jnp.zeros_like(v)
        us, ys, rs, ss = [], [], [], []
        for k in range(8):
            r = lax.rsqrt(spread(c[k][k : k + 1, :]))
            u = spread(v[k : k + 1, :]) * r
            w = spread(y[k : k + 1, :]) * r
            upper = jnp.where(sub == k, u, upper)
            inverse = jnp.where(sub == k, w, inverse)
            low = jnp.where(sub > k, c[k], 0.0) * r
            if k < 7:
                v = v - low * u
                y = y - low * w
            scaled = {}
            for m in range(k + 1, 8):
                scaled[m] = spread(c[m][k : k + 1, :]) * r
                c[m] = c[m] - low * scaled[m]
            us.append(u)
            ys.append(w)
            rs.append(r)
            ss.append(scaled)
        uppers.append(upper)
        inverses.append(inverse)
        for g in range(b + 1, groups):
            cg = [spread(rows[g][:, 8 * b + m : 8 * b + m + 1]) for m in range(8)]
            ag, wg = rows[g], inv[g]
            for k in range(8):
                low = cg[k] * rs[k]
                for m in range(k + 1, 8):
                    cg[m] = cg[m] - low * ss[k][m]
                ag = ag - low * us[k]
                wg = wg - low * ys[k]
            rows[g], inv[g] = ag, wg
    return uppers, inverses


def factor_block(work_ref, tile_ref, out_ref, log_ref):
    lane = lax.broadcasted_iota(jnp.int32, (8, TILE), 1)
    sub = lax.broadcasted_iota(jnp.int32, (8, TILE), 0)
    work_ref[:, NB:] = jnp.where(
        lax.broadcasted_iota(jnp.int32, (NB, NB), 0) == lax.broadcasted_iota(jnp.int32, (NB, NB), 1), 1.0, 0.0
    ).astype(jnp.float32)
    log_ref[...] = jnp.zeros_like(log_ref)
    out_ref[...] = jnp.zeros_like(out_ref)

    @pl.loop(0, NB // TILE)
    def _(t):
        o = pl.multiple_of(t * TILE, TILE)
        live = pl.ds(o, NB + TILE)
        uppers, inverses = factor_tile(work_ref[pl.ds(o, TILE), pl.ds(o, TILE)])
        logs = jnp.zeros((8, TILE), jnp.float32)
        for g in range(TILE // 8):
            tile_ref[8 * g : 8 * g + 8, :] = inverses[g]
            logs = logs + jnp.where(lane == sub + 8 * g, jnp.log(jnp.where(lane == sub + 8 * g, uppers[g], 1.0)), 0.0)
        log_ref[...] += logs
        out_ref[pl.ds(o, TILE), live] = mm(tile_ref[...], work_ref[pl.ds(o, TILE), live])

        @pl.loop(t + 1, NB // TILE)
        def _(i):
            q = pl.multiple_of(i * TILE, TILE)
            work_ref[pl.ds(q, TILE), live] -= mm(
                out_ref[pl.ds(o, TILE), pl.ds(q, TILE)], out_ref[pl.ds(o, TILE), live], TN
            )

        for g in range(TILE // 8):
            out_ref[pl.ds(pl.multiple_of(o + 8 * g, 8), 8), pl.ds(o, TILE)] = jnp.where(
                lane >= sub + 8 * g, uppers[g], 0.0
            )


def place_parts(dst_ref, parts_ref, x):
    for t in range(NX):
        q = lax.rem(x - t + NX, NX)
        dst_ref[:, pl.ds(pl.multiple_of(q * TILE, TILE), TILE)] = parts_ref[:, t * TILE : (t + 1) * TILE]


def first_kernel(a_ref, out_ref, log_ref, work_ref, tile_ref):
    half = NB // 2
    rows = half // (2 * NX)
    work_ref[half:, :half] = jnp.zeros((half, half), jnp.float32)
    for r in range(2 * NX):
        o = (r % 2 * NX + r // 2) * rows
        work_ref[o : o + rows, :NB] = a_ref[r * rows : (r + 1) * rows, :NB]
        work_ref[half + o : half + o + rows, half:NB] = a_ref[r * rows : (r + 1) * rows, NB:]
    factor_block(work_ref, tile_ref, out_ref, log_ref)


def second_kernel(where_ref, own_ref, other_ref, first_ref, out_ref, right_ref, log_ref, work_ref, tile_ref, sort_ref):
    x, south = where_ref[0], where_ref[1] == 0
    sort_ref[...] = jnp.where(south, own_ref[...], other_ref[...])
    place_parts(work_ref, sort_ref, x)
    right_ref[...] = mm(first_ref[:, NB:], work_ref[:, :NB])
    sort_ref[...] = jnp.where(south, other_ref[...], own_ref[...])
    place_parts(work_ref, sort_ref, x)
    work_ref[:, :NB] -= mm(right_ref[...], right_ref[...], TN)
    factor_block(work_ref, tile_ref, out_ref, log_ref)


def vmem_specs(count):
    return [pl.BlockSpec(memory_space=pltpu.VMEM)] * count


SMEM_SPEC = pl.BlockSpec(memory_space=pltpu.SMEM)


def first_block(a):
    return pl.pallas_call(
        first_kernel,
        out_shape=(jax.ShapeDtypeStruct((NB, 2 * NB), jnp.float32), jax.ShapeDtypeStruct((8, TILE), jnp.float32)),
        in_specs=vmem_specs(1),
        out_specs=vmem_specs(2),
        scratch_shapes=[pltpu.VMEM((NB, 2 * NB), jnp.float32), pltpu.VMEM((TILE, TILE), jnp.float32)],
        compiler_params=pltpu.CompilerParams(vmem_limit_bytes=VMEM_LIMIT),
        cost_estimate=pl.CostEstimate(flops=2 * 10**9, bytes_accessed=3 * 2**20, transcendentals=0),
        name="first_block",
    )(a)


def second_block(where, own, other, first):
    return pl.pallas_call(
        second_kernel,
        out_shape=(
            jax.ShapeDtypeStruct((NB, 2 * NB), jnp.float32),
            jax.ShapeDtypeStruct((NB, NB), jnp.float32),
            jax.ShapeDtypeStruct((8, TILE), jnp.float32),
        ),
        in_specs=[SMEM_SPEC] + vmem_specs(3),
        out_specs=vmem_specs(3),
        scratch_shapes=[
            pltpu.VMEM((NB, 2 * NB), jnp.float32),
            pltpu.VMEM((TILE, TILE), jnp.float32),
            pltpu.VMEM((NB, NB), jnp.float32),
        ],
        compiler_params=pltpu.CompilerParams(vmem_limit_bytes=VMEM_LIMIT),
        cost_estimate=pl.CostEstimate(flops=2 * 10**9, bytes_accessed=5 * 2**20, transcendentals=0),
        name="second_block",
    )(where, own, other, first)


def halves(value):
    high = value.astype(jnp.bfloat16)
    return high, (value - high.astype(jnp.float32)).astype(jnp.bfloat16)


def dot3(a, b):
    def dot(p, q):
        return lax.dot_general(p, q, NN, preferred_element_type=jnp.float32)

    return dot(a[0], b[0]) + (dot(a[0], b[1]) + dot(a[1], b[0]))


def solve_kernel(where_ref, *refs):
    parts, (first_ref, right_ref, second_ref, out_ref) = refs[:NX], refs[NX:]
    x, core, col = where_ref[0], where_ref[1], where_ref[2]
    sources = (first_ref[...], second_ref[...], right_ref[...])
    split = [halves(value) for value in sources + tuple(value.T for value in sources)]

    def times(n, value):
        return dot3(split[n], halves(value))

    value = jnp.concatenate([part[...] for part in parts], axis=1)
    top = times(0, value[:NB])
    bottom = times(1, value[NB:] - times(5, top))
    row = lax.broadcasted_iota(jnp.int32, (NB, TILE), 0)
    column = lax.broadcasted_iota(jnp.int32, (NB, TILE), 1)
    places, tops, bottoms = [], [], []
    first_panel, second_panel = jnp.logical_and(core == 0, col == 0), jnp.logical_and(core == 0, col == 1)
    for n in range(NX):
        place = pl.multiple_of(lax.rem(x - n + NX, NX) * TILE, TILE)
        unit = jnp.where(row == column + place, -1.0, 0.0).astype(jnp.float32)
        lanes = slice(n * TILE, (n + 1) * TILE)
        tops.append(jnp.where(first_panel, unit, jnp.where(second_panel, 0.0, top[:, lanes])))
        bottoms.append(jnp.where(second_panel, unit, jnp.where(first_panel, 0.0, bottom[:, lanes])))
        places.append(place)
    bottom = times(4, jnp.concatenate(bottoms, axis=1))
    top = times(3, jnp.concatenate(tops, axis=1) - times(2, bottom))
    for block, value in enumerate((top, bottom)):
        for n, place in enumerate(places):
            out_ref[block * NB : (block + 1) * NB, pl.ds(place, TILE)] = value[:, n * TILE : (n + 1) * TILE]


def solve(where, parts, first, right, second):
    whole = pl.BlockSpec(parts[0].shape, lambda j, w: (0, 0))
    inverse = pl.BlockSpec((NB, NB), lambda j, w: (0, 1))
    square = pl.BlockSpec((NB, NB), lambda j, w: (0, 0))
    return pl.pallas_call(
        solve_kernel,
        out_shape=jax.ShapeDtypeStruct((2 * NB, NB), jnp.float32),
        grid_spec=pltpu.PrefetchScalarGridSpec(
            num_scalar_prefetch=1,
            grid=(1,),
            in_specs=[whole] * NX + [inverse, square, inverse],
            out_specs=pl.BlockSpec((2 * NB, NB), lambda j, w: (0, 0)),
        ),
        compiler_params=pltpu.CompilerParams(vmem_limit_bytes=VMEM_LIMIT),
        cost_estimate=pl.CostEstimate(flops=3 * 10**9, bytes_accessed=7 * 2**20, transcendentals=0),
        name="solve",
    )(where, *parts, first, right, second)


def update_kernel(
    where_ref, matrix_ref, left0_ref, left1_ref, own_ref, other_ref, first_ref, second_ref, out_ref, split_ref
):
    core, col, row = where_ref[1], where_ref[2], where_ref[3]
    step = pl.program_id(0)
    rows, columns = out_ref.shape

    @pl.when(step == 0)
    def _():
        own, other = own_ref[...], other_ref[...]
        for block, value in enumerate((jnp.where(core == 0, own, other), jnp.where(core == 0, other, own))):
            lanes = slice(block * NB, (block + 1) * NB)
            high, low = halves(value)
            split_ref[: 2 * NB, lanes] = high
            split_ref[2 * NB : 4 * NB, lanes] = low
            split_ref[4 * NB :, lanes] = high

    high0, low0 = halves(left0_ref[...])
    high1, low1 = halves(left1_ref[...])
    left = jnp.concatenate([high0, high1, high0, high1, low0, low1], axis=1)
    product = lax.dot_general(left, split_ref[...], NN, preferred_element_type=jnp.float32)
    out_ref[:, NB:] = matrix_ref[:, NB:] - product[:, NB:]
    out_ref[:, :NB] = jnp.where(col < 2, 0.0, matrix_ref[:, :NB]) - product[:, :NB]

    @pl.when(jnp.logical_and(row < 2, step < NB // rows))
    def _():
        out_ref[:, NB:] = jnp.zeros((rows, columns - NB), jnp.float32)

        @pl.when(jnp.logical_not(jnp.logical_and(row == 1, col == 0)))
        def _():
            out_ref[:, :NB] = jnp.zeros((rows, NB), jnp.float32)

        @pl.when(row == col)
        def _():
            o = pl.multiple_of(step * rows, rows)
            u = jnp.where(col == 0, first_ref[:, pl.ds(o, rows)], second_ref[:, pl.ds(o, rows)])
            keep = lax.broadcasted_iota(jnp.int32, (NB, rows), 0) <= (
                lax.broadcasted_iota(jnp.int32, (NB, rows), 1) + o
            )
            out_ref[:, :NB] = jnp.where(keep, u, 0.0).T


def update(where, matrix, left, own, other, first, second):
    rows, columns = matrix.shape
    tile = 256

    def whole(value):
        return pl.BlockSpec(value.shape, lambda i, w: (0, 0))

    square = pl.BlockSpec((NB, NB), lambda i, w: (0, 0))
    return pl.pallas_call(
        update_kernel,
        out_shape=jax.ShapeDtypeStruct((rows, columns), jnp.float32),
        grid_spec=pltpu.PrefetchScalarGridSpec(
            num_scalar_prefetch=1,
            grid=(rows // tile,),
            in_specs=[
                pl.BlockSpec((tile, columns), lambda i, w: (i, 0)),
                pl.BlockSpec((tile, NB), lambda i, w: (i, 0)),
                pl.BlockSpec((tile, NB), lambda i, w: (i, 0)),
                whole(own),
                whole(other),
                square,
                square,
            ],
            out_specs=pl.BlockSpec((tile, columns), lambda i, w: (i, 0)),
            scratch_shapes=[pltpu.VMEM((6 * NB, columns), jnp.bfloat16)],
        ),
        compiler_params=pltpu.CompilerParams(vmem_limit_bytes=VMEM_LIMIT),
        cost_estimate=pl.CostEstimate(flops=12 * 10**9, bytes_accessed=28 * 2**20, transcendentals=0),
        name="update",
    )(where, matrix, *left, own, other, first, second)


def per_device(stored):
    row, col = lax.axis_index("row"), lax.axis_index("col")
    x, core = row // 2, row % 2
    z, y = col // NY, col % NY
    where = jnp.stack([x, core, col, row]).astype(jnp.int32)
    slab = stored[:, :NB]
    corner = slab[:NB]
    plane = [(zz, yy) for zz in range(NZ) for yy in range(NY)]
    both = (0, 1)

    half = NB // 2
    rows = half // (2 * NX)
    block = jnp.concatenate([corner[:half], corner[half:, half:]], axis=1)
    other = send(block[half // 2 :], [(device(0, 0, 0, 0), device(0, 1, 0, 0))])
    block = jnp.where(core == 0, block[: half // 2], other)
    chunks = [block[t * rows : (t + 1) * rows] for t in range(NX)]
    p0 = scatter_x(chunks, [(0, 0)])
    p0 = pick(x == 0, chunks[0], p0)
    p0_y = spread_y(p0, both, 0)
    left = [jnp.where(col == number, stored[:, :NB], 0.0) for number in range(2)]
    left = lax.psum(left, "col")
    p0 = pick(y == 0, p0, p0_y)
    p0_z = spread_z(p0, both)
    p0 = pick(z == 0, p0, p0_z)
    p0 = lax.all_gather(p0, "row", axis=0, tiled=True)

    strip = stored[:NB]
    chunks = [
        jnp.concatenate([strip[:, t * TILE : (t + 1) * TILE], strip[:, NB + t * TILE : NB + (t + 1) * TILE]], axis=1)
        for t in range(NX)
    ]
    quarter_x = scatter_x(chunks, plane)
    quarter = pick(x == 0, chunks[0], quarter_x)
    near, far = quarter[:, :TILE], quarter[:, TILE:]
    given = swap_core(jnp.where(core == 0, far, near), both)
    a1_y = spread_y(near, both, 1)
    a1 = pick(y == 1, near, a1_y)
    a1_z = spread_z(a1, both)
    a1 = pick(z == 0, a1, a1_z)
    a1_parts = gather_x(a1, both)
    first, log0 = first_block(p0)
    a1 = jnp.concatenate(a1_parts, axis=1)
    a1_other = swap_core(a1, both)
    kept = jnp.where(core == 0, near, far)
    right_part = jnp.where(core == 0, jnp.concatenate([kept, given], axis=0), jnp.concatenate([given, kept], axis=0))
    right_parts = gather_x(right_part, both)
    second, right, log1 = second_block(where, a1, a1_other, first)
    own = solve(where, right_parts, first, right, second)
    other = swap_core(own, both)
    matrix = update(where, stored, left, own, other, first, second)
    log_total = 2.0 * jnp.sum(log0 + log1)
    return matrix, log_total


def solution(mesh):
    return jax.shard_map(
        per_device, mesh=mesh, in_specs=(P("row", "col"),), out_specs=(P("row", "col"), P()), check_vma=False
    )
```

```python
import jax
import jax.numpy as jnp
from jax import lax
from jax.experimental import pallas as pl
from jax.experimental.pallas import tpu as pltpu
from jax.sharding import PartitionSpec as P

NB = 512
TILE = 128
NX, NY, NZ = 4, 4, 4
HI = lax.Precision.HIGHEST
NN = (((1,), (0,)), ((), ()))
TN = (((0,), (0,)), ((), ()))
VMEM_LIMIT = 60 * 2**20


def mm(a, b, dims=NN):
    return lax.dot_general(a, b, dims, precision=HI, preferred_element_type=jnp.float32)


def device(x, core, z, y):
    return (2 * x + core) * (NZ * NY) + z * NY + y


def send(value, pairs):
    return lax.ppermute(value, ("row", "col"), pairs)


def scatter_x(chunks, ys):
    return [
        send(chunks[t], [(device(0, k, z, y), device(t, k, z, y)) for k in range(2) for z, y in ys])
        for t in range(1, NX)
    ]


def spread_y(value, cores, source):
    return [
        send(
            value,
            [(device(x, k, 0, source), device(x, k, 0, (source + t) % NY)) for x in range(NX) for k in cores],
        )
        for t in range(1, NY)
    ]


def spread_z(value, cores):
    return [
        send(
            value,
            [(device(x, k, 0, y), device(x, k, t, y)) for x in range(NX) for k in cores for y in range(NY)],
        )
        for t in range(1, NZ)
    ]


def gather_x(value, cores):
    return [value] + [
        send(
            value,
            [
                (device(x, k, z, y), device((x + t) % NX, k, z, y))
                for x in range(NX)
                for k in cores
                for z in range(NZ)
                for y in range(NY)
            ],
        )
        for t in range(1, NX)
    ]


def swap_core(value, cores):
    return send(
        value,
        [
            (device(x, k, z, y), device(x, 1 - k, z, y))
            for x in range(NX)
            for k in cores
            for z in range(NZ)
            for y in range(NY)
        ],
    )


def pick(mine, own, received):
    total = received[0]
    for other in received[1:]:
        total = total + other
    return jnp.where(mine, own, total)


def spread(x):
    return jnp.broadcast_to(x, (8, TILE))


def factor_tile(a):
    sub = lax.broadcasted_iota(jnp.int32, (8, TILE), 0)
    lane = lax.broadcasted_iota(jnp.int32, (8, TILE), 1)
    groups = TILE // 8
    rows = [a[8 * g : 8 * g + 8, :] for g in range(groups)]
    inv = [jnp.where(lane == sub + 8 * g, 1.0, 0.0).astype(jnp.float32) for g in range(groups)]
    uppers, inverses = [], []
    for b in range(groups):
        v, y = rows[b], inv[b]
        c = [spread(v[:, 8 * b + m : 8 * b + m + 1]) for m in range(8)]
        upper, inverse = jnp.zeros_like(v), jnp.zeros_like(v)
        us, ys, rs, ss = [], [], [], []
        for k in range(8):
            r = lax.rsqrt(spread(c[k][k : k + 1, :]))
            u = spread(v[k : k + 1, :]) * r
            w = spread(y[k : k + 1, :]) * r
            upper = jnp.where(sub == k, u, upper)
            inverse = jnp.where(sub == k, w, inverse)
            low = jnp.where(sub > k, c[k], 0.0) * r
            if k < 7:
                v = v - low * u
                y = y - low * w
            scaled = {}
            for m in range(k + 1, 8):
                scaled[m] = spread(c[m][k : k + 1, :]) * r
                c[m] = c[m] - low * scaled[m]
            us.append(u)
            ys.append(w)
            rs.append(r)
            ss.append(scaled)
        uppers.append(upper)
        inverses.append(inverse)
        for g in range(b + 1, groups):
            cg = [spread(rows[g][:, 8 * b + m : 8 * b + m + 1]) for m in range(8)]
            ag, wg = rows[g], inv[g]
            for k in range(8):
                low = cg[k] * rs[k]
                for m in range(k + 1, 8):
                    cg[m] = cg[m] - low * ss[k][m]
                ag = ag - low * us[k]
                wg = wg - low * ys[k]
            rows[g], inv[g] = ag, wg
    return uppers, inverses


def factor_block(work_ref, tile_ref, out_ref, log_ref):
    lane = lax.broadcasted_iota(jnp.int32, (8, TILE), 1)
    sub = lax.broadcasted_iota(jnp.int32, (8, TILE), 0)
    work_ref[:, NB:] = jnp.where(
        lax.broadcasted_iota(jnp.int32, (NB, NB), 0) == lax.broadcasted_iota(jnp.int32, (NB, NB), 1), 1.0, 0.0
    ).astype(jnp.float32)
    log_ref[...] = jnp.zeros_like(log_ref)
    out_ref[...] = jnp.zeros_like(out_ref)

    @pl.loop(0, NB // TILE)
    def _(t):
        o = pl.multiple_of(t * TILE, TILE)
        live = pl.ds(o, NB + TILE)
        uppers, inverses = factor_tile(work_ref[pl.ds(o, TILE), pl.ds(o, TILE)])
        logs = jnp.zeros((8, TILE), jnp.float32)
        for g in range(TILE // 8):
            tile_ref[8 * g : 8 * g + 8, :] = inverses[g]
            logs = logs + jnp.where(lane == sub + 8 * g, jnp.log(jnp.where(lane == sub + 8 * g, uppers[g], 1.0)), 0.0)
        log_ref[...] += logs
        out_ref[pl.ds(o, TILE), live] = mm(tile_ref[...], work_ref[pl.ds(o, TILE), live])

        @pl.loop(t + 1, NB // TILE)
        def _(i):
            q = pl.multiple_of(i * TILE, TILE)
            work_ref[pl.ds(q, TILE), live] -= mm(
                out_ref[pl.ds(o, TILE), pl.ds(q, TILE)], out_ref[pl.ds(o, TILE), live], TN
            )

        for g in range(TILE // 8):
            out_ref[pl.ds(pl.multiple_of(o + 8 * g, 8), 8), pl.ds(o, TILE)] = jnp.where(
                lane >= sub + 8 * g, uppers[g], 0.0
            )


def place_parts(dst_ref, parts_ref, x):
    for t in range(NX):
        q = lax.rem(x - t + NX, NX)
        dst_ref[:, pl.ds(pl.multiple_of(q * TILE, TILE), TILE)] = parts_ref[:, t * TILE : (t + 1) * TILE]


def first_kernel(a_ref, out_ref, log_ref, work_ref, tile_ref):
    half = NB // 2
    rows = half // (2 * NX)
    work_ref[half:, :half] = jnp.zeros((half, half), jnp.float32)
    for r in range(2 * NX):
        o = (r % 2 * NX + r // 2) * rows
        work_ref[o : o + rows, :NB] = a_ref[r * rows : (r + 1) * rows, :NB]
        work_ref[half + o : half + o + rows, half:NB] = a_ref[r * rows : (r + 1) * rows, NB:]
    factor_block(work_ref, tile_ref, out_ref, log_ref)


def second_kernel(where_ref, own_ref, other_ref, first_ref, out_ref, right_ref, log_ref, work_ref, tile_ref, sort_ref):
    x, south = where_ref[0], where_ref[1] == 0
    sort_ref[...] = jnp.where(south, own_ref[...], other_ref[...])
    place_parts(work_ref, sort_ref, x)
    right_ref[...] = mm(first_ref[:, NB:], work_ref[:, :NB])
    sort_ref[...] = jnp.where(south, other_ref[...], own_ref[...])
    place_parts(work_ref, sort_ref, x)
    work_ref[:, :NB] -= mm(right_ref[...], right_ref[...], TN)
    factor_block(work_ref, tile_ref, out_ref, log_ref)


def vmem_specs(count):
    return [pl.BlockSpec(memory_space=pltpu.VMEM)] * count


SMEM_SPEC = pl.BlockSpec(memory_space=pltpu.SMEM)


def first_block(a):
    return pl.pallas_call(
        first_kernel,
        out_shape=(jax.ShapeDtypeStruct((NB, 2 * NB), jnp.float32), jax.ShapeDtypeStruct((8, TILE), jnp.float32)),
        in_specs=vmem_specs(1),
        out_specs=vmem_specs(2),
        scratch_shapes=[pltpu.VMEM((NB, 2 * NB), jnp.float32), pltpu.VMEM((TILE, TILE), jnp.float32)],
        compiler_params=pltpu.CompilerParams(vmem_limit_bytes=VMEM_LIMIT),
        cost_estimate=pl.CostEstimate(flops=2 * 10**9, bytes_accessed=3 * 2**20, transcendentals=0),
        name="first_block",
    )(a)


def second_block(where, own, other, first):
    return pl.pallas_call(
        second_kernel,
        out_shape=(
            jax.ShapeDtypeStruct((NB, 2 * NB), jnp.float32),
            jax.ShapeDtypeStruct((NB, NB), jnp.float32),
            jax.ShapeDtypeStruct((8, TILE), jnp.float32),
        ),
        in_specs=[SMEM_SPEC] + vmem_specs(3),
        out_specs=vmem_specs(3),
        scratch_shapes=[
            pltpu.VMEM((NB, 2 * NB), jnp.float32),
            pltpu.VMEM((TILE, TILE), jnp.float32),
            pltpu.VMEM((NB, NB), jnp.float32),
        ],
        compiler_params=pltpu.CompilerParams(vmem_limit_bytes=VMEM_LIMIT),
        cost_estimate=pl.CostEstimate(flops=2 * 10**9, bytes_accessed=5 * 2**20, transcendentals=0),
        name="second_block",
    )(where, own, other, first)


def halves(value):
    high = value.astype(jnp.bfloat16)
    return high, (value - high.astype(jnp.float32)).astype(jnp.bfloat16)


def dot3(a, b):
    def dot(p, q):
        return lax.dot_general(p, q, NN, preferred_element_type=jnp.float32)

    return dot(a[0], b[0]) + (dot(a[0], b[1]) + dot(a[1], b[0]))


def solve_kernel(where_ref, *refs):
    parts, (first_ref, right_ref, second_ref, out_ref) = refs[:NX], refs[NX:]
    x, core, col = where_ref[0], where_ref[1], where_ref[2]
    sources = (first_ref[...], second_ref[...], right_ref[...])
    split = [halves(value) for value in sources + tuple(value.T for value in sources)]

    def times(n, value):
        return dot3(split[n], halves(value))

    value = jnp.concatenate([part[...] for part in parts], axis=1)
    top = times(0, value[:NB])
    bottom = times(1, value[NB:] - times(5, top))
    row = lax.broadcasted_iota(jnp.int32, (NB, TILE), 0)
    column = lax.broadcasted_iota(jnp.int32, (NB, TILE), 1)
    places, tops, bottoms = [], [], []
    first_panel, second_panel = jnp.logical_and(core == 0, col == 0), jnp.logical_and(core == 0, col == 1)
    for n in range(NX):
        place = pl.multiple_of(lax.rem(x - n + NX, NX) * TILE, TILE)
        unit = jnp.where(row == column + place, -1.0, 0.0).astype(jnp.float32)
        lanes = slice(n * TILE, (n + 1) * TILE)
        tops.append(jnp.where(first_panel, unit, jnp.where(second_panel, 0.0, top[:, lanes])))
        bottoms.append(jnp.where(second_panel, unit, jnp.where(first_panel, 0.0, bottom[:, lanes])))
        places.append(place)
    bottom = times(4, jnp.concatenate(bottoms, axis=1))
    top = times(3, jnp.concatenate(tops, axis=1) - times(2, bottom))
    for block, value in enumerate((top, bottom)):
        for n, place in enumerate(places):
            out_ref[block * NB : (block + 1) * NB, pl.ds(place, TILE)] = value[:, n * TILE : (n + 1) * TILE]


def solve(where, parts, first, right, second):
    whole = pl.BlockSpec(parts[0].shape, lambda j, w: (0, 0))
    inverse = pl.BlockSpec((NB, NB), lambda j, w: (0, 1))
    square = pl.BlockSpec((NB, NB), lambda j, w: (0, 0))
    return pl.pallas_call(
        solve_kernel,
        out_shape=jax.ShapeDtypeStruct((2 * NB, NB), jnp.float32),
        grid_spec=pltpu.PrefetchScalarGridSpec(
            num_scalar_prefetch=1,
            grid=(1,),
            in_specs=[whole] * NX + [inverse, square, inverse],
            out_specs=pl.BlockSpec((2 * NB, NB), lambda j, w: (0, 0)),
        ),
        compiler_params=pltpu.CompilerParams(vmem_limit_bytes=VMEM_LIMIT),
        cost_estimate=pl.CostEstimate(flops=3 * 10**9, bytes_accessed=7 * 2**20, transcendentals=0),
        name="solve",
    )(where, *parts, first, right, second)


def update_kernel(
    where_ref, matrix_ref, left0_ref, left1_ref, own_ref, other_ref, first_ref, second_ref, out_ref, split_ref
):
    core, col, row = where_ref[1], where_ref[2], where_ref[3]
    step = pl.program_id(0)
    rows, columns = out_ref.shape

    @pl.when(step == 0)
    def _():
        own, other = own_ref[...], other_ref[...]
        for block, value in enumerate((jnp.where(core == 0, own, other), jnp.where(core == 0, other, own))):
            lanes = slice(block * NB, (block + 1) * NB)
            split_ref[0, :, lanes], split_ref[1, :, lanes] = halves(value)

    def times(left_ref, half):
        lines = pl.ds(half * NB, NB)
        return dot3(halves(left_ref[...]), (split_ref[0, lines, :], split_ref[1, lines, :]))

    product = times(left0_ref, 0) + times(left1_ref, 1)
    out_ref[:, NB:] = matrix_ref[:, NB:] - product[:, NB:]
    out_ref[:, :NB] = jnp.where(col < 2, 0.0, matrix_ref[:, :NB]) - product[:, :NB]

    @pl.when(jnp.logical_and(row < 2, step < NB // rows))
    def _():
        out_ref[:, NB:] = jnp.zeros((rows, columns - NB), jnp.float32)

        @pl.when(jnp.logical_not(jnp.logical_and(row == 1, col == 0)))
        def _():
            out_ref[:, :NB] = jnp.zeros((rows, NB), jnp.float32)

        @pl.when(row == col)
        def _():
            o = pl.multiple_of(step * rows, rows)
            u = jnp.where(col == 0, first_ref[:, pl.ds(o, rows)], second_ref[:, pl.ds(o, rows)])
            keep = lax.broadcasted_iota(jnp.int32, (NB, rows), 0) <= (
                lax.broadcasted_iota(jnp.int32, (NB, rows), 1) + o
            )
            out_ref[:, :NB] = jnp.where(keep, u, 0.0).T


def update(where, matrix, left, own, other, first, second):
    rows, columns = matrix.shape
    tile = 256

    def whole(value):
        return pl.BlockSpec(value.shape, lambda i, w: (0, 0))

    square = pl.BlockSpec((NB, NB), lambda i, w: (0, 0))
    return pl.pallas_call(
        update_kernel,
        out_shape=jax.ShapeDtypeStruct((rows, columns), jnp.float32),
        grid_spec=pltpu.PrefetchScalarGridSpec(
            num_scalar_prefetch=1,
            grid=(rows // tile,),
            in_specs=[
                pl.BlockSpec((tile, columns), lambda i, w: (i, 0)),
                pl.BlockSpec((tile, NB), lambda i, w: (i, 0)),
                pl.BlockSpec((tile, NB), lambda i, w: (i, 0)),
                whole(own),
                whole(other),
                square,
                square,
            ],
            out_specs=pl.BlockSpec((tile, columns), lambda i, w: (i, 0)),
            scratch_shapes=[pltpu.VMEM((2, 2 * NB, columns), jnp.bfloat16)],
        ),
        compiler_params=pltpu.CompilerParams(vmem_limit_bytes=VMEM_LIMIT),
        cost_estimate=pl.CostEstimate(flops=12 * 10**9, bytes_accessed=28 * 2**20, transcendentals=0),
        name="update",
    )(where, matrix, *left, own, other, first, second)


def per_device(stored):
    row, col = lax.axis_index("row"), lax.axis_index("col")
    x, core = row // 2, row % 2
    z, y = col // NY, col % NY
    where = jnp.stack([x, core, col, row]).astype(jnp.int32)
    slab = stored[:, :NB]
    corner = slab[:NB]
    plane = [(zz, yy) for zz in range(NZ) for yy in range(NY)]
    both = (0, 1)

    half = NB // 2
    rows = half // (2 * NX)
    block = jnp.concatenate([corner[:half], corner[half:, half:]], axis=1)
    other = send(block[half // 2 :], [(device(0, 0, 0, 0), device(0, 1, 0, 0))])
    block = jnp.where(core == 0, block[: half // 2], other)
    chunks = [block[t * rows : (t + 1) * rows] for t in range(NX)]
    p0 = scatter_x(chunks, [(0, 0)])
    p0 = pick(x == 0, chunks[0], p0)
    p0_y = spread_y(p0, both, 0)
    left = [jnp.where(col == number, stored[:, :NB], 0.0) for number in range(2)]
    left = lax.psum(left, "col")
    p0 = pick(y == 0, p0, p0_y)
    p0_z = spread_z(p0, both)
    p0 = pick(z == 0, p0, p0_z)
    p0 = lax.all_gather(p0, "row", axis=0, tiled=True)

    strip = stored[:NB]
    chunks = [
        jnp.concatenate([strip[:, t * TILE : (t + 1) * TILE], strip[:, NB + t * TILE : NB + (t + 1) * TILE]], axis=1)
        for t in range(NX)
    ]
    quarter_x = scatter_x(chunks, plane)
    quarter = pick(x == 0, chunks[0], quarter_x)
    near, far = quarter[:, :TILE], quarter[:, TILE:]
    given = swap_core(jnp.where(core == 0, far, near), both)
    a1_y = spread_y(near, both, 1)
    a1 = pick(y == 1, near, a1_y)
    a1_z = spread_z(a1, both)
    a1 = pick(z == 0, a1, a1_z)
    a1_parts = gather_x(a1, both)
    first, log0 = first_block(p0)
    a1 = jnp.concatenate(a1_parts, axis=1)
    a1_other = swap_core(a1, both)
    kept = jnp.where(core == 0, near, far)
    right_part = jnp.where(core == 0, jnp.concatenate([kept, given], axis=0), jnp.concatenate([given, kept], axis=0))
    right_parts = gather_x(right_part, both)
    second, right, log1 = second_block(where, a1, a1_other, first)
    own = solve(where, right_parts, first, right, second)
    other = swap_core(own, both)
    matrix = update(where, stored, left, own, other, first, second)
    log_total = 2.0 * jnp.sum(log0 + log1)
    return matrix, log_total


def solution(mesh):
    return jax.shard_map(
        per_device, mesh=mesh, in_specs=(P("row", "col"),), out_specs=(P("row", "col"), P()), check_vma=False
    )
```
